32 devices in a mesh: dp: 1, ep: 32 (over x, y, z, core).
Axes of the slice: x: 2, y: 2, z: 4, core: 2. Of those that a mesh axis runs over, the one named last changes fastest.
Arguments:
- x: bfloat16 [1, 32, 256, 1792], P('dp', 'ep')
- expert: int32 [1, 32, 256, 8], P('dp', 'ep')
- slot: int32 [1, 32, 256, 8], P('dp', 'ep')
- gate: float32 [1, 32, 256, 8], P('dp', 'ep')
- w_gate: bfloat16 [96, 1792, 2048], P('ep')
- w_up: bfloat16 [96, 1792, 2048], P('ep')
- w_down: bfloat16 [96, 2048, 1792], P('ep')
- s_gate: bfloat16 [1792, 2048], replicated
- s_up: bfloat16 [1792, 2048], replicated
- s_down: bfloat16 [2048, 1792], replicated
Outputs:
- y: bfloat16 [1, 32, 256, 1792], P('dp', 'ep')
All inputs are finite; a program needn't handle non-finite values.
Results may differ from the reference program's by a relative error of at most 0.009.
Values are sent between devices in bfloat16 or wider.
A program may use at most 2 GiB of HBM per device.

```python
import jax
import jax.numpy as jnp

MEMBERS = 32
TOKENS = 256
D = 1792
FF = 2048
TOP = 8
EXPERTS = 96
SHARED_FF = 2048
SLOTS = 5 * TOKENS * TOP // (4 * EXPERTS)


def setup_inputs(seed: int = 0, part: int = 0) -> dict:
    own, k1, k2, k3, k4, k5, k6 = jax.random.split(jax.random.key(seed), 7)
    kx, ke, kl, kg = jax.random.split(jax.random.fold_in(own, part), 4)
    devices = (1, MEMBERS)
    place = jax.random.permutation(kl, jnp.arange(EXPERTS, dtype=jnp.uint32))
    slow = ((EXPERTS + (9 * place) % EXPERTS) << ((9 * place) // EXPERTS)) // EXPERTS
    wait = (jax.random.bits(ke, (*devices, TOKENS, EXPERTS), jnp.uint32) >> 10) * slow
    expert = jnp.argsort(wait, axis=-1)[..., :TOP].astype(jnp.int32)
    chosen = jax.nn.one_hot(expert, EXPERTS, dtype=jnp.int32)
    in_line = jnp.cumsum(chosen.reshape(*devices, TOKENS * TOP, EXPERTS), axis=2) - 1
    slot = jnp.sum(in_line.reshape(chosen.shape) * chosen, axis=-1)

    def one(key, rows, columns):
        return (jax.random.normal(key, (rows, columns), jnp.float32) * rows**-0.5).astype(jnp.bfloat16)

    def weights(key, rows, columns):
        return jax.lax.map(lambda k: one(k, rows, columns), jax.random.split(key, EXPERTS))

    return {
        "x": jax.random.normal(kx, (*devices, TOKENS, D), jnp.float32).astype(jnp.bfloat16),
        "expert": expert,
        "slot": slot,
        "gate": jax.nn.softmax(jax.random.normal(kg, expert.shape, jnp.float32)),
        "w_gate": weights(k1, D, FF),
        "w_up": weights(k2, D, FF),
        "w_down": weights(k3, FF, D),
        "s_gate": one(k4, D, SHARED_FF),
        "s_up": one(k5, D, SHARED_FF),
        "s_down": one(k6, SHARED_FF, D),
    }


def einsum(form, a, b):
    return jnp.einsum(form, a.astype(jnp.float32), b.astype(jnp.float32))


def for_all(x, s_gate, s_up, s_down):
    h = jax.nn.silu(einsum("...d,df->...f", x, s_gate)) * einsum("...d,df->...f", x, s_up)
    return einsum("...f,fd->...d", h.astype(jnp.bfloat16), s_down)


def reference(x, expert, slot, gate, w_gate, w_up, w_down, s_gate, s_up, s_down):
    to_expert = jax.nn.one_hot(expert, EXPERTS, dtype=jnp.bfloat16)
    to_slot = jax.nn.one_hot(slot, SLOTS, dtype=jnp.bfloat16)
    weighted = to_expert * gate[..., None].astype(jnp.bfloat16)
    dispatch = einsum("abtke,abtkc->abtec", to_expert, to_slot).astype(jnp.bfloat16)
    combine = einsum("abtke,abtkc->abtec", weighted, to_slot).astype(jnp.bfloat16)
    z = einsum("abtec,abtd->aebcd", dispatch, x).astype(jnp.bfloat16)
    h = jax.nn.silu(einsum("aebcd,edf->aebcf", z, w_gate))
    h = (h * einsum("aebcd,edf->aebcf", z, w_up)).astype(jnp.bfloat16)
    out = einsum("aebcf,efd->aebcd", h, w_down).astype(jnp.bfloat16)
    y = einsum("abtec,aebcd->abtd", combine, out)
    return (y + for_all(x, s_gate, s_up, s_down)).astype(jnp.bfloat16)
```

```python
import jax
import jax.numpy as jnp
from jax import lax
from jax.sharding import PartitionSpec as P

F32, BF16 = jnp.float32, jnp.bfloat16


def dot(form, a, b):
    return jnp.einsum(form, a, b, preferred_element_type=F32)


def solution(mesh):
    def step(x, expert, slot, gate, w_gate, w_up, w_down, s_gate, s_up, s_down):
        tokens, top = expert.shape[2:]
        members = mesh.shape["ep"]
        own = w_gate.shape[0]
        slots = 5 * tokens * top // (4 * own * members)
        x0 = x[0, 0]
        table = jnp.concatenate(
            [
                expert[0, 0].astype(BF16),
                jnp.minimum(slot[0, 0], slots).astype(BF16),
                gate[0, 0].astype(BF16),
            ],
            axis=1,
        ).T
        xs = lax.all_gather(x0, "ep")
        ts = lax.all_gather(table, "ep")
        first = lax.axis_index("ep") * own
        e = ts[:, :top].astype(jnp.int32) - first
        c = ts[:, top : 2 * top].astype(jnp.int32)
        g = ts[:, 2 * top :]
        rows = own * slots
        pos = jnp.where((e >= 0) & (e < own) & (c < slots), e * slots + c, rows)
        hit = pos[:, :, None, :] == lax.broadcasted_iota(jnp.int32, (1, 1, rows, 1), 2)
        pick = jnp.any(hit, axis=1).astype(BF16)
        weigh = jnp.sum(jnp.where(hit, g[:, :, None, :].astype(F32), 0.0), axis=1).astype(BF16)
        z = dot("spt,std->spd", pick, xs).astype(BF16)
        z = z.reshape(members, own, slots, -1).transpose(1, 0, 2, 3).reshape(own, members * slots, -1)
        h = jax.nn.silu(dot("emd,edf->emf", z, w_gate)) * dot("emd,edf->emf", z, w_up)
        out = dot("emf,efd->emd", h.astype(BF16), w_down).astype(BF16)
        out = out.reshape(own, members, slots, -1).transpose(1, 0, 2, 3).reshape(members, rows, -1)
        part = dot("spt,spd->std", weigh, out).astype(BF16)
        y = lax.psum_scatter(part, "ep", scatter_dimension=0, tiled=False)
        h = jax.nn.silu(dot("td,df->tf", x0, s_gate)) * dot("td,df->tf", x0, s_up)
        shared = dot("tf,fd->td", h.astype(BF16), s_down)
        return (y.astype(F32) + shared).astype(BF16)[None, None]

    row = P("dp", "ep", None, None)
    w = P("ep", None, None)
    s = P(None, None)
    return jax.shard_map(
        step, mesh=mesh, in_specs=(row, row, row, row, w, w, w, s, s, s), out_specs=row, check_vma=False
    )
```

```python
import functools

import jax
import jax.numpy as jnp
from jax import lax
from jax.experimental import pallas as pl
from jax.experimental.pallas import tpu as pltpu
from jax.sharding import PartitionSpec as P

F32, BF16, I32 = jnp.float32, jnp.bfloat16, jnp.int32
MESH = pl.DeviceIdType.MESH

SLOTS = 26
PLANE = 8
LINE = 4
OWN = 3
BLOCKS = OWN * PLANE
PAD = 32
START = (0, 24, 48, 72)
ROWS = (24, 24, 24, 32)
BACK = ((0, 0, 24), (1, 0, 24), (2, 0, 24), (3, 0, 16), (3, 16, 16))
HALF = 16
COLS = 256
WIDE = 512
DEEP_F, DEEP_D = 3, 4
CALLS = 1 + LINE * OWN


def loop(n, body):
    lax.fori_loop(0, n, lambda i, c: (body(i), c)[1], 0)


def kernel(
    x, tab, w_gate, w_up, w_down, s_gate, s_up, s_down, y,
    lines, tabs, staged, slots, back, terms, shared, hidden, pick, pick_next, fbuf, dbuf,
    z_send, z_recv, d_send, d_recv, r_send, r_recv, p_send, p_recv, f_sem, d_sem,
):
    me = lax.axis_index("ep")
    mx, my, mz, mc = me // 16, (me // 8) % 2, (me // 2) % 4, me % 2
    place = (me // 8) * 2 + mc
    depth = x.shape[1]
    nf, nd = s_gate.shape[1] // WIDE, depth // COLS

    def peer(j):
        px, py, pc = (mx + j // 4) % 2, (my + (j // 2) % 2) % 2, (mc + j % 2) % 2
        return {"ep": ((px * 2 + py) * 4 + mz) * 2 + pc}, (px * 2 + py) * 2 + pc

    def line_peer(o):
        pz = (mz + 1 - 2 * (mz % 2), (mz + 2) % 4, 3 - mz)[o - 1]
        return {"ep": ((mx * 2 + my) * 4 + pz) * 2 + mc}

    def wide(ref, i):
        return ref.at[:, pl.ds(pl.multiple_of(i * WIDE, WIDE), WIDE)]

    def narrow(ref, i):
        return ref.at[:, pl.ds(pl.multiple_of(i * COLS, COLS), COLS)]

    def f_copies(gate, up, i, s):
        return [
            pltpu.make_async_copy(wide(gate, i), fbuf.at[s, 0], f_sem.at[s, 0]),
            pltpu.make_async_copy(wide(up, i), fbuf.at[s, 1], f_sem.at[s, 1]),
        ]

    def start_f(g):
        n, i, s = g // nf, g % nf, g % DEEP_F

        @pl.when(n == 0)
        def _():
            for c in f_copies(s_gate, s_up, i, s):
                c.start()

        @pl.when((n > 0) & (n < CALLS))
        def _():
            e = (n + OWN - 1) % OWN
            for c in f_copies(w_gate.at[e], w_up.at[e], i, s):
                c.start()

    def start_d(g):
        n, i, s = g // nd, g % nd, g % DEEP_D

        @pl.when(n == 0)
        def _():
            pltpu.make_async_copy(narrow(s_down, i), dbuf.at[s], d_sem.at[s]).start()

        @pl.when((n > 0) & (n < CALLS))
        def _():
            e = (n + OWN - 1) % OWN
            pltpu.make_async_copy(narrow(w_down.at[e], i), dbuf.at[s], d_sem.at[s]).start()

    loop(DEEP_F, start_f)
    loop(DEEP_D, start_d)

    barrier = pltpu.get_barrier_semaphore()
    for o in range(1, LINE):
        pl.semaphore_signal(barrier, inc=1, device_id=line_peer(o), device_id_type=MESH)
    for j in range(1, PLANE):
        pl.semaphore_signal(barrier, inc=1, device_id=peer(j)[0], device_id_type=MESH)
    pl.semaphore_wait(barrier, LINE - 1 + PLANE - 1)

    def line_copies(o):
        return [
            pltpu.make_async_remote_copy(
                src_ref=src, dst_ref=dst.at[o - 1], send_sem=z_send.at[o - 1, i], recv_sem=z_recv.at[o - 1, i],
                device_id=line_peer(o), device_id_type=MESH,
            )
            for i, (src, dst) in enumerate(((tab, tabs), (x, lines)))
        ]

    for o in range(1, LINE):
        for c in line_copies(o):
            c.start()

    def build(ref, height, o, start, rows, weigh):
        table = tab if o == 0 else tabs.at[o - 1]
        code = table[0:8, :].astype(I32) - mz * 1024
        gates = table[8:16, :]
        r = lax.broadcasted_iota(I32, (height, code.shape[1]), 0)
        v = r + (start - SLOTS * o)
        ok = (v >= 0) & (v < SLOTS) & (r < rows)

        def block(b):
            want = jnp.where(ok, v + b * SLOTS, -7)
            acc = jnp.zeros(want.shape, F32)
            for i in range(8):
                value = gates[i : i + 1, :] if weigh else jnp.float32(1)
                acc = jnp.where(want == code[i : i + 1, :], value, acc)
            ref[pl.ds(pl.multiple_of(b * height, height), height), :] = acc.astype(BF16)

        loop(BLOCKS, block)

    def tokens_of(o):
        return x if o == 0 else lines.at[o - 1]

    def slot_copy(k, j):
        device, there = peer(j)
        return pltpu.make_async_remote_copy(
            src_ref=staged.at[k, :, there, 0 : ROWS[k]], dst_ref=slots.at[k, :, place, 0 : ROWS[k]],
            send_sem=d_send.at[k, j], recv_sem=d_recv.at[k, j], device_id=device, device_id_type=MESH,
        )

    def dispatch(k):
        if k:
            for c in line_copies(k):
                c.wait_recv()
        build(pick.at[0], PAD, k, START[k], ROWS[k], False)
        if k:
            build(pick.at[1], PAD, k - 1, START[k], ROWS[k], False)

        def columns(i):
            c = pl.ds(pl.multiple_of(i * COLS, COLS), COLS)
            out = jnp.dot(pick[0], tokens_of(k)[:, c], preferred_element_type=F32)
            if k:
                out += jnp.dot(pick[1], tokens_of(k - 1)[:, c], preferred_element_type=F32)
            staged[k, :, :, :, c] = out.astype(BF16).reshape(OWN, PLANE, PAD, COLS)

        loop(nd, columns)
        loop(PLANE - 1, lambda i: slot_copy(k, PLANE - 1 - i).start())
        slots[k, :, place] = staged[k, :, place]

    def ffn(n, read, write):
        def up(i):
            g = n * nf + i
            s = g % DEEP_F
            for c in f_copies(s_gate, s_up, 0, s):
                c.wait()
            z = read()
            a = jnp.dot(z, fbuf[s, 0], preferred_element_type=F32)
            b = jnp.dot(z, fbuf[s, 1], preferred_element_type=F32)
            hidden[:, pl.ds(pl.multiple_of(i * WIDE, WIDE), WIDE)] = (a * jax.nn.sigmoid(a) * b).astype(BF16)
            start_f(g + DEEP_F)

        def down(i):
            g = n * nd + i
            s = g % DEEP_D
            pltpu.make_async_copy(narrow(s_down, 0), dbuf.at[s], d_sem.at[s]).wait()
            write(
                pl.ds(pl.multiple_of(i * COLS, COLS), COLS),
                jnp.dot(hidden[...], dbuf[s], preferred_element_type=F32),
            )
            start_d(g + DEEP_D)

        loop(nf, up)
        loop(nd, down)

    def back_copy(p, j):
        k, r, rows = BACK[p]
        device, there = peer(j)
        return pltpu.make_async_remote_copy(
            src_ref=staged.at[k, :, there, r : r + rows], dst_ref=back.at[k, :, place, r : r + rows],
            send_sem=r_send.at[p, j], recv_sem=r_recv.at[p, j], device_id=device, device_id_type=MESH,
        )

    def send_back(p):
        loop(PLANE - 1, lambda i: back_copy(p, PLANE - 1 - i).start())
        k, r, rows = BACK[p]
        back[k, :, place, r : r + rows] = staged[k, :, place, r : r + rows]

    def term_copy(o):
        return pltpu.make_async_remote_copy(
            src_ref=lines.at[o - 1], dst_ref=terms.at[o - 1], send_sem=p_send.at[o - 1], recv_sem=p_recv.at[o - 1],
            device_id=line_peer(o), device_id_type=MESH,
        )

    for k in range(LINE - 1):
        back[k, :, :, ROWS[k] : PAD] = jnp.zeros((OWN, PLANE, PAD - ROWS[k], depth), BF16)

    dispatch(0)

    def write_shared(c, value):
        shared[:, c] = value

    ffn(0, lambda: x[...], write_shared)
    dispatch(1)

    def call(m):
        n = m + 1
        k, e = m // OWN, m % OWN
        for kk in range(LINE):
            @pl.when(m == kk * OWN)
            def _():
                def wait(i):
                    c = slot_copy(kk, i + 1)
                    c.wait_recv()
                    c.wait_send()

                loop(PLANE - 1, wait)

        def write(c, value):
            staged[k, e, :, :, c] = value.astype(BF16).reshape(PLANE, PAD, COLS)

        ffn(n, lambda: slots[k, e].reshape(PLANE * PAD, depth), write)

        @pl.when(m == 1)
        def _():
            dispatch(2)

        @pl.when(m == 5)
        def _():
            dispatch(3)

        @pl.when(m == 8)
        def _():
            send_back(2)

    loop(LINE * OWN, call)
    for p in (3, 4, 1, 0):
        send_back(p)

    def combine(o, pieces, write):
        for p in pieces:
            loop(PLANE - 1, lambda i: back_copy(p, i + 1).wait_recv())
        build(pick.at[0], PAD, o, START[o], ROWS[o], True)
        if o < LINE - 1:
            build(pick_next, HALF, o, START[o + 1], HALF, True)

        def columns(i):
            c = pl.ds(pl.multiple_of(i * COLS, COLS), COLS)

            def dot(weights, rows):
                return lax.dot_general(weights, rows, (((0,), (0,)), ((), ())), preferred_element_type=F32)

            out = dot(pick[0], back[o, :, :, :, c].reshape(BLOCKS * PAD, COLS))
            if o < LINE - 1:
                out += dot(pick_next[...], back[o + 1, :, :, 0:HALF, c].reshape(BLOCKS * HALF, COLS))
            write(c, out)

        loop(nd, columns)

    def keep(o):
        def write(c, value):
            lines[o - 1, :, c] = value.astype(BF16)

        return write

    for o, pieces in ((2, (2, 3)), (3, (4,)), (1, (1,))):
        for c in line_copies(o):
            c.wait_send()
        combine(o, pieces, keep(o))
        term_copy(o).start()

    def finish(c, value):
        for o in range(1, LINE):
            value += terms[o - 1, :, c].astype(F32)
        y[:, c] = (value + shared[:, c]).astype(BF16)

    loop(PLANE - 1, lambda i: back_copy(0, i + 1).wait_recv())
    for o in range(1, LINE):
        term_copy(o).wait()
    combine(0, (), finish)
    for p in range(len(BACK)):
        loop(PLANE - 1, lambda i: back_copy(p, i + 1).wait_send())


def solution(mesh):
    def step(x, expert, slot, gate, w_gate, w_up, w_down, s_gate, s_up, s_down):
        tokens, depth = x.shape[2:]
        width = s_gate.shape[1]
        dev, e = expert[0, 0] // OWN, expert[0, 0] % OWN
        place = (dev // 8) * 2 + dev % 2
        code = ((dev // 2) % 4) * 1024 + (e * PLANE + place) * SLOTS + slot[0, 0]
        code = jnp.where(slot[0, 0] < SLOTS, code, -1)
        tab = jnp.concatenate([code.T.astype(F32), gate[0, 0].T], axis=0)
        vmem = pl.BlockSpec(memory_space=pltpu.VMEM)
        hbm = pl.BlockSpec(memory_space=pl.ANY)
        dma = pltpu.SemaphoreType.DMA
        rows = PLANE * PAD
        y = pl.pallas_call(
            kernel,
            name="moe",
            out_shape=jax.ShapeDtypeStruct((tokens, depth), BF16),
            in_specs=[vmem, vmem] + [hbm] * 6,
            out_specs=vmem,
            scratch_shapes=[
                pltpu.VMEM((LINE - 1, tokens, depth), BF16),
                pltpu.VMEM((LINE - 1, 16, tokens), F32),
                pltpu.VMEM((LINE, OWN, PLANE, PAD, depth), BF16),
                pltpu.VMEM((LINE, OWN, PLANE, PAD, depth), BF16),
                pltpu.VMEM((LINE, OWN, PLANE, PAD, depth), BF16),
                pltpu.VMEM((LINE - 1, tokens, depth), BF16),
                pltpu.VMEM((tokens, depth), F32),
                pltpu.VMEM((rows, width), BF16),
                pltpu.VMEM((2, BLOCKS * PAD, tokens), BF16),
                pltpu.VMEM((BLOCKS * HALF, tokens), BF16),
                pltpu.VMEM((DEEP_F, 2, depth, WIDE), BF16),
                pltpu.VMEM((DEEP_D, width, COLS), BF16),
                dma((LINE - 1, 2)), dma((LINE - 1, 2)),
                dma((LINE, PLANE)), dma((LINE, PLANE)),
                dma((len(BACK), PLANE)), dma((len(BACK), PLANE)),
                dma((LINE - 1,)), dma((LINE - 1,)),
                dma((DEEP_F, 2)), dma((DEEP_D,)),
            ],
            compiler_params=pltpu.CompilerParams(
                collective_id=0, has_side_effects=True, vmem_limit_bytes=67043328
            ),
        )(x[0, 0], tab, w_gate, w_up, w_down, s_gate, s_up, s_down)
        return y[None, None]

    row = P("dp", "ep", None, None)
    w = P("ep", None, None)
    s = P(None, None)
    return jax.shard_map(
        step, mesh=mesh, in_specs=(row, row, row, row, w, w, w, s, s, s), out_specs=row, check_vma=False
    )
```

```python
import functools

import jax
import jax.numpy as jnp
from jax import lax
from jax.experimental import pallas as pl
from jax.experimental.pallas import tpu as pltpu
from jax.sharding import PartitionSpec as P

F32, BF16, I32 = jnp.float32, jnp.bfloat16, jnp.int32
MESH = pl.DeviceIdType.MESH


def scoped(name, call):
    with jax.named_scope(name):
        call()


SLOTS = 26
PLANE = 8
LINE = 4
OWN = 3
BLOCKS = OWN * PLANE
PAD = 32
START = (0, 24, 48, 72)
ROWS = (24, 24, 24, 32)
BACK = ((0, 0, 24), (1, 0, 24), (2, 0, 24), (3, 0, 16), (3, 16, 16))
HALF = 16
COLS = 256
WIDE = 512
DEEP_F, DEEP_D = 3, 3
CALLS = 1 + LINE * OWN


def loop(n, body):
    lax.fori_loop(0, n, lambda i, c: (body(i), c)[1], 0)


def kernel(
    x, tab, w_gate, w_up, w_down, s_gate, s_up, s_down, y,
    lines, tabs, staged, slots, back, terms, shared, hidden, pick, pick_next, fbuf, dbuf,
    z_send, z_recv, d_send, d_recv, r_send, r_recv, p_send, p_recv, f_sem, d_sem,
):
    me = lax.axis_index("ep")
    mx, my, mz, mc = me // 16, (me // 8) % 2, (me // 2) % 4, me % 2
    place = (me // 8) * 2 + mc
    depth = x.shape[1]
    nf, nc = s_gate.shape[1] // WIDE, depth // COLS
    whole, tail = depth // WIDE, depth % WIDE
    nd = whole + (tail > 0)
    middle = (mz > 0) & (mz < 3)

    def peer(j):
        px, py, pc = (mx + j // 4) % 2, (my + (j // 2) % 2) % 2, (mc + j % 2) % 2
        return {"ep": ((px * 2 + py) * 4 + mz) * 2 + pc}, (px * 2 + py) * 2 + pc

    def line_peer(o):
        pz = (mz + 1 - 2 * (mz % 2), (mz + 2) % 4, 3 - mz)[o - 1]
        return {"ep": ((mx * 2 + my) * 4 + pz) * 2 + mc}

    def wide(ref, i):
        return ref.at[:, pl.ds(pl.multiple_of(i * WIDE, WIDE), WIDE)]

    def d_copy(ref, i, s):
        return pltpu.make_async_copy(wide(ref, i), dbuf.at[s], d_sem.at[s])

    def d_tail(ref, s):
        return pltpu.make_async_copy(ref.at[:, whole * WIDE :], dbuf.at[s, :, 0:tail], d_sem.at[s])

    def f_copies(gate, up, i, s):
        return [
            pltpu.make_async_copy(wide(gate, i), fbuf.at[s, 0], f_sem.at[s, 0]),
            pltpu.make_async_copy(wide(up, i), fbuf.at[s, 1], f_sem.at[s, 1]),
        ]

    def start_f(g):
        n, i, s = g // nf, g % nf, g % DEEP_F

        @pl.when(n == 0)
        def _():
            for c in f_copies(s_gate, s_up, i, s):
                c.start()

        @pl.when((n > 0) & (n < CALLS))
        def _():
            e = (n + OWN - 1) % OWN
            for c in f_copies(w_gate.at[e], w_up.at[e], i, s):
                c.start()

    def start_d(g):
        n, i, s = g // nd, g % nd, g % DEEP_D

        def start(ref):
            @pl.when(i < whole)
            def _():
                d_copy(ref, i, s).start()

            if tail:
                @pl.when(i == whole)
                def _():
                    d_tail(ref, s).start()

        @pl.when(n == 0)
        def _():
            start(s_down)

        @pl.when((n > 0) & (n < CALLS))
        def _():
            start(w_down.at[(n + OWN - 1) % OWN])

    loop(DEEP_F, start_f)
    loop(DEEP_D, start_d)

    barrier = pltpu.get_barrier_semaphore()
    for o in range(1, LINE):
        pl.semaphore_signal(barrier, inc=1, device_id=line_peer(o), device_id_type=MESH)
    for j in range(1, PLANE):
        pl.semaphore_signal(barrier, inc=1, device_id=peer(j)[0], device_id_type=MESH)
    def line_copies(q, src, to, slot):
        pairs = ((tab, x),) + tuple((tabs.at[o], lines.at[o]) for o in range(LINE - 1))
        return [
            pltpu.make_async_remote_copy(
                src_ref=ref, dst_ref=dst.at[slot - 1], send_sem=z_send.at[q, i], recv_sem=z_recv.at[slot - 1, i],
                device_id=line_peer(to), device_id_type=MESH,
            )
            for i, (ref, dst) in enumerate(zip(pairs[src], (tabs, lines)))
        ]

    LINE_SENDS = ((0, 1, 1), (0, 3, 3), (1, 3, 2), (3, 1, 2), (2, 1, 3))

    def line_start(q):
        for c in line_copies(q, *LINE_SENDS[q]):
            c.start()

    def line_wait(o):
        for c in line_copies(0, 0, o, o):
            c.wait_recv()

    def build(ref, height, o, start, rows, weigh):
        table = tab if o == 0 else tabs.at[o - 1]
        code = table[0:8, :].astype(I32) - mz * 1024
        gates = table[8:16, :]
        r = lax.broadcasted_iota(I32, (height, code.shape[1]), 0)
        v = r + (start - SLOTS * o)
        ok = (v >= 0) & (v < SLOTS) & (r < rows)

        def block(b):
            want = jnp.where(ok, v + b * SLOTS, -7)
            acc = jnp.zeros(want.shape, F32)
            for i in range(8):
                value = gates[i : i + 1, :] if weigh else jnp.float32(1)
                acc = jnp.where(want == code[i : i + 1, :], value, acc)
            ref[pl.ds(pl.multiple_of(b * height, height), height), :] = acc.astype(BF16)

        loop(BLOCKS, block)

    def tokens_of(o):
        return x if o == 0 else lines.at[o - 1]

    def slot_copy(k, j):
        device, there = peer(j)
        return pltpu.make_async_remote_copy(
            src_ref=staged.at[k, :, there, 0 : ROWS[k]], dst_ref=slots.at[k, :, place, 0 : ROWS[k]],
            send_sem=d_send.at[k, j], recv_sem=d_recv.at[k, j], device_id=device, device_id_type=MESH,
        )

    def stage(k):
        build(pick.at[0], PAD, k, START[k], ROWS[k], False)
        if k:
            build(pick.at[1], PAD, k - 1, START[k], ROWS[k], False)

        def columns(i):
            c = pl.ds(pl.multiple_of(i * COLS, COLS), COLS)
            out = jnp.dot(pick[0], tokens_of(k)[:, c], preferred_element_type=F32)
            if k:
                out += jnp.dot(pick[1], tokens_of(k - 1)[:, c], preferred_element_type=F32)
            staged[k, :, :, :, c] = out.astype(BF16).reshape(OWN, PLANE, PAD, COLS)

        loop(nc, columns)

    def dispatch(k):
        loop(PLANE - 1, lambda i: slot_copy(k, PLANE - 1 - i).start())
        slots[k, :, place] = staged[k, :, place]

    def ffn(n, read, write):
        def up(i):
            g = n * nf + i
            s = g % DEEP_F
            for c in f_copies(s_gate, s_up, 0, s):
                c.wait()
            z = read()
            a = jnp.dot(z, fbuf[s, 0], preferred_element_type=F32)
            b = jnp.dot(z, fbuf[s, 1], preferred_element_type=F32)
            hidden[:, pl.ds(pl.multiple_of(i * WIDE, WIDE), WIDE)] = (a * jax.nn.sigmoid(a) * b).astype(BF16)
            start_f(g + DEEP_F)

        def down(i):
            g = n * nd + i
            s = g % DEEP_D
            d_copy(s_down, 0, s).wait()
            write(
                pl.ds(pl.multiple_of(i * WIDE, WIDE), WIDE),
                jnp.dot(hidden[...], dbuf[s], preferred_element_type=F32),
            )
            start_d(g + DEEP_D)

        scoped("up", lambda: loop(nf, up))
        scoped("down", lambda: loop(whole, down))
        if tail:
            g = n * nd + whole
            s = g % DEEP_D
            d_tail(s_down, s).wait()
            write(
                pl.ds(whole * WIDE, tail),
                jnp.dot(hidden[...], dbuf[s, :, 0:tail], preferred_element_type=F32),
            )
            start_d(g + DEEP_D)

    def back_copy(p, j):
        k, r, rows = BACK[p]
        device, there = peer(j)
        return pltpu.make_async_remote_copy(
            src_ref=staged.at[k, :, there, r : r + rows], dst_ref=back.at[k, :, place, r : r + rows],
            send_sem=r_send.at[p, j], recv_sem=r_recv.at[p, j], device_id=device, device_id_type=MESH,
        )

    def send_back(p):
        loop(PLANE - 1, lambda i: back_copy(p, PLANE - 1 - i).start())
        k, r, rows = BACK[p]
        back[k, :, place, r : r + rows] = staged[k, :, place, r : r + rows]

    def term_copy(o):
        return pltpu.make_async_remote_copy(
            src_ref=lines.at[o - 1], dst_ref=terms.at[o - 1], send_sem=p_send.at[o - 1], recv_sem=p_recv.at[o - 1],
            device_id=line_peer(o), device_id_type=MESH,
        )

    for k in range(LINE - 1):
        back[k, :, :, ROWS[k] : PAD] = jnp.zeros((OWN, PLANE, PAD - ROWS[k], depth), BF16)

    stage(0)
    scoped("barrier", lambda: pl.semaphore_wait(barrier, LINE - 1 + PLANE - 1))
    line_start(0)

    @pl.when(middle)
    def _():
        line_start(1)

    dispatch(0)

    def write_shared(c, value):
        shared[:, c] = value

    ffn(0, lambda: x[...], write_shared)
    scoped("wait_line1", lambda: line_wait(1))

    @pl.when(middle)
    def _():
        line_start(2)
        scoped("wait_line3m", lambda: line_wait(3))
        line_start(3)

    stage(1)
    dispatch(1)

    def call(m):
        n = m + 1
        k, e = m // OWN, m % OWN
        for kk in range(LINE):
            @pl.when(m == kk * OWN)
            def _():
                def wait(i):
                    c = slot_copy(kk, i + 1)
                    c.wait_recv()
                    c.wait_send()

                scoped(f"wait_slots{kk}", lambda: loop(PLANE - 1, wait))

        def write(c, value):
            staged[k, e, :, :, c] = value.astype(BF16).reshape(PLANE, PAD, value.shape[1])

        ffn(n, lambda: slots[k, e].reshape(PLANE * PAD, depth), write)

        @pl.when(m == 1)
        def _():
            scoped("wait_line2", lambda: line_wait(2))

            @pl.when(middle)
            def _():
                line_start(4)

            stage(2)
            dispatch(2)

        @pl.when(m == 4)
        def _():
            @pl.when((mz == 0) | (mz == 3))
            def _():
                scoped("wait_line3e", lambda: line_wait(3))

            stage(3)
            dispatch(3)

        @pl.when(m == 8)
        def _():
            send_back(2)

    loop(LINE * OWN, call)
    for p in (3, 4, 1, 0):
        send_back(p)

    def combine(o, pieces, write, wait=lambda: None):
        build(pick.at[0], PAD, o, START[o], ROWS[o], True)
        if o < LINE - 1:
            build(pick_next, HALF, o, START[o + 1], HALF, True)
        for p in pieces:
            scoped(f"wait_back{p}", lambda: loop(PLANE - 1, lambda i: back_copy(p, i + 1).wait_recv()))
        scoped(f"wait_terms{o}", wait)

        def columns(i):
            c = pl.ds(pl.multiple_of(i * COLS, COLS), COLS)

            def dot(weights, rows):
                return lax.dot_general(weights, rows, (((0,), (0,)), ((), ())), preferred_element_type=F32)

            out = dot(pick[0], back[o, :, :, :, c].reshape(BLOCKS * PAD, COLS))
            if o < LINE - 1:
                out += dot(pick_next[...], back[o + 1, :, :, 0:HALF, c].reshape(BLOCKS * HALF, COLS))
            write(c, out)

        loop(nc, columns)

    def keep(o):
        def write(c, value):
            lines[o - 1, :, c] = value.astype(BF16)

        return write

    for c in line_copies(0, *LINE_SENDS[0]):
        c.wait_send()

    @pl.when(middle)
    def _():
        for q in range(1, len(LINE_SENDS)):
            for c in line_copies(q, *LINE_SENDS[q]):
                c.wait_send()

    for o, pieces in ((2, (2, 3)), (3, (4,)), (1, (1,))):
        combine(o, pieces, keep(o))
        term_copy(o).start()

    def finish(c, value):
        for o in range(1, LINE):
            value += terms[o - 1, :, c].astype(F32)
        y[:, c] = (value + shared[:, c]).astype(BF16)

    combine(0, (0,), finish, lambda: [term_copy(o).wait() for o in (2, 3, 1)])
    for p in range(len(BACK)):
        loop(PLANE - 1, lambda i: back_copy(p, i + 1).wait_send())


def solution(mesh):
    def step(x, expert, slot, gate, w_gate, w_up, w_down, s_gate, s_up, s_down):
        tokens, depth = x.shape[2:]
        width = s_gate.shape[1]
        dev, e = expert[0, 0] // OWN, expert[0, 0] % OWN
        place = (dev // 8) * 2 + dev % 2
        code = ((dev // 2) % 4) * 1024 + (e * PLANE + place) * SLOTS + slot[0, 0]
        code = jnp.where(slot[0, 0] < SLOTS, code, -1)
        tab = jnp.concatenate([code.T.astype(F32), gate[0, 0].T], axis=0)
        vmem = pl.BlockSpec(memory_space=pltpu.VMEM)
        hbm = pl.BlockSpec(memory_space=pl.ANY)
        dma = pltpu.SemaphoreType.DMA
        rows = PLANE * PAD
        y = pl.pallas_call(
            kernel,
            name="moe",
            out_shape=jax.ShapeDtypeStruct((tokens, depth), BF16),
            in_specs=[vmem, vmem] + [hbm] * 6,
            out_specs=vmem,
            scratch_shapes=[
                pltpu.VMEM((LINE - 1, tokens, depth), BF16),
                pltpu.VMEM((LINE - 1, 16, tokens), F32),
                pltpu.VMEM((LINE, OWN, PLANE, PAD, depth), BF16),
                pltpu.VMEM((LINE, OWN, PLANE, PAD, depth), BF16),
                pltpu.VMEM((LINE, OWN, PLANE, PAD, depth), BF16),
                pltpu.VMEM((LINE - 1, tokens, depth), BF16),
                pltpu.VMEM((tokens, depth), F32),
                pltpu.VMEM((rows, width), BF16),
                pltpu.VMEM((2, BLOCKS * PAD, tokens), BF16),
                pltpu.VMEM((BLOCKS * HALF, tokens), BF16),
                pltpu.VMEM((DEEP_F, 2, depth, WIDE), BF16),
                pltpu.VMEM((DEEP_D, width, WIDE), BF16),
                dma((5, 2)), dma((LINE - 1, 2)),
                dma((LINE, PLANE)), dma((LINE, PLANE)),
                dma((len(BACK), PLANE)), dma((len(BACK), PLANE)),
                dma((LINE - 1,)), dma((LINE - 1,)),
                dma((DEEP_F, 2)), dma((DEEP_D,)),
            ],
            compiler_params=pltpu.CompilerParams(
                collective_id=0, has_side_effects=True, vmem_limit_bytes=67043328
            ),
        )(x[0, 0], tab, w_gate, w_up, w_down, s_gate, s_up, s_down)
        return y[None, None]

    row = P("dp", "ep", None, None)
    w = P("ep", None, None)
    s = P(None, None)
    return jax.shard_map(
        step, mesh=mesh, in_specs=(row, row, row, row, w, w, w, s, s, s), out_specs=row, check_vma=False
    )
```

```python
import functools

import jax
import jax.numpy as jnp
from jax import lax
from jax.experimental import pallas as pl
from jax.experimental.pallas import tpu as pltpu
from jax.sharding import PartitionSpec as P

F32, BF16, I32 = jnp.float32, jnp.bfloat16, jnp.int32
MESH = pl.DeviceIdType.MESH


def scoped(name, call):
    with jax.named_scope(name):
        call()


SLOTS = 26
PLANE = 8
LINE = 4
OWN = 3
BLOCKS = OWN * PLANE
PAD = 32
START = (0, 24, 48, 72)
ROWS = (24, 24, 24, 32)
BACK = ((0, 0, 24), (1, 0, 24), (2, 0, 24), (3, 0, 16), (3, 16, 16))
HALF = 16
COLS = 256
WIDE = 512
DEEP_F, DEEP_D = 3, 3
CALLS = 1 + LINE * OWN


def loop(n, body):
    lax.fori_loop(0, n, lambda i, c: (body(i), c)[1], 0)


def kernel(
    x, tab, w_gate, w_up, w_down, s_gate, s_up, s_down, y,
    lines, tabs, staged, slots, back, terms, shared, hidden, pick, pick_next, fbuf, dbuf,
    z_send, z_recv, d_send, d_recv, r_send, r_recv, p_send, p_recv, f_sem, d_sem,
):
    me = lax.axis_index("ep")
    mx, my, mz, mc = me // 16, (me // 8) % 2, (me // 2) % 4, me % 2
    place = (me // 8) * 2 + mc
    depth = x.shape[1]
    nf, nc = s_gate.shape[1] // WIDE, depth // COLS
    whole, tail = depth // WIDE, depth % WIDE
    nd = whole + (tail > 0)
    middle = (mz > 0) & (mz < 3)

    def peer(j):
        px, py, pc = (mx + j // 4) % 2, (my + (j // 2) % 2) % 2, (mc + j % 2) % 2
        return {"ep": ((px * 2 + py) * 4 + mz) * 2 + pc}, (px * 2 + py) * 2 + pc

    def line_peer(o):
        pz = (mz + 1 - 2 * (mz % 2), (mz + 2) % 4, 3 - mz)[o - 1]
        return {"ep": ((mx * 2 + my) * 4 + pz) * 2 + mc}

    def wide(ref, i):
        return ref.at[:, pl.ds(pl.multiple_of(i * WIDE, WIDE), WIDE)]

    def d_copy(ref, i, s):
        return pltpu.make_async_copy(wide(ref, i), dbuf.at[s], d_sem.at[s])

    def d_tail(ref, s):
        return pltpu.make_async_copy(ref.at[:, whole * WIDE :], dbuf.at[s, :, 0:tail], d_sem.at[s])

    def f_copies(gate, up, i, s):
        return [
            pltpu.make_async_copy(wide(gate, i), fbuf.at[s, 0], f_sem.at[s, 0]),
            pltpu.make_async_copy(wide(up, i), fbuf.at[s, 1], f_sem.at[s, 1]),
        ]

    def start_f(g):
        n, i, s = g // nf, g % nf, g % DEEP_F

        @pl.when(n == 0)
        def _():
            for c in f_copies(s_gate, s_up, i, s):
                c.start()

        @pl.when((n > 0) & (n < CALLS))
        def _():
            e = (n + OWN - 1) % OWN
            for c in f_copies(w_gate.at[e], w_up.at[e], i, s):
                c.start()

    def start_d(g):
        n, i, s = g // nd, g % nd, g % DEEP_D

        def start(ref):
            @pl.when(i < whole)
            def _():
                d_copy(ref, i, s).start()

            if tail:
                @pl.when(i == whole)
                def _():
                    d_tail(ref, s).start()

        @pl.when(n == 0)
        def _():
            start(s_down)

        @pl.when((n > 0) & (n < CALLS))
        def _():
            start(w_down.at[(n + OWN - 1) % OWN])

    loop(DEEP_F, start_f)
    loop(DEEP_D, start_d)

    barrier = pltpu.get_barrier_semaphore()
    for o in range(1, LINE):
        pl.semaphore_signal(barrier, inc=1, device_id=line_peer(o), device_id_type=MESH)
    for j in range(1, PLANE):
        pl.semaphore_signal(barrier, inc=1, device_id=peer(j)[0], device_id_type=MESH)
    def line_copies(q, src, to, slot):
        pairs = ((tab, x),) + tuple((tabs.at[o], lines.at[o]) for o in range(LINE - 1))
        return [
            pltpu.make_async_remote_copy(
                src_ref=ref, dst_ref=dst.at[slot - 1], send_sem=z_send.at[q, i], recv_sem=z_recv.at[slot - 1, i],
                device_id=line_peer(to), device_id_type=MESH,
            )
            for i, (ref, dst) in enumerate(zip(pairs[src], (tabs, lines)))
        ]

    LINE_SENDS = ((0, 1, 1), (0, 3, 3), (1, 3, 2), (3, 1, 2), (2, 1, 3))

    def line_start(q):
        for c in line_copies(q, *LINE_SENDS[q]):
            c.start()

    def line_wait(o):
        for c in line_copies(0, 0, o, o):
            c.wait_recv()

    def build(ref, height, o, start, rows, weigh):
        table = tab if o == 0 else tabs.at[o - 1]
        code = table[0:8, :].astype(I32) - mz * 1024
        gates = table[8:16, :]
        r = lax.broadcasted_iota(I32, (height, code.shape[1]), 0)
        v = r + (start - SLOTS * o)
        ok = (v >= 0) & (v < SLOTS) & (r < rows)

        def block(b):
            want = jnp.where(ok, v + b * SLOTS, -7)
            acc = jnp.zeros(want.shape, F32)
            for i in range(8):
                value = gates[i : i + 1, :] if weigh else jnp.float32(1)
                acc = jnp.where(want == code[i : i + 1, :], value, acc)
            ref[pl.ds(pl.multiple_of(b * height, height), height), :] = acc.astype(BF16)

        loop(BLOCKS, block)

    def tokens_of(o):
        return x if o == 0 else lines.at[o - 1]

    def slot_copy(k, j):
        device, there = peer(j)
        return pltpu.make_async_remote_copy(
            src_ref=staged.at[k, :, there, 0 : ROWS[k]], dst_ref=slots.at[k, :, place, 0 : ROWS[k]],
            send_sem=d_send.at[k, j], recv_sem=d_recv.at[k, j], device_id=device, device_id_type=MESH,
        )

    def stage(k):
        build(pick.at[0], PAD, k, START[k], ROWS[k], False)
        if k:
            build(pick.at[1], PAD, k - 1, START[k], ROWS[k], False)

        def columns(i):
            c = pl.ds(pl.multiple_of(i * COLS, COLS), COLS)
            out = jnp.dot(pick[0], tokens_of(k)[:, c], preferred_element_type=F32)
            if k:
                out += jnp.dot(pick[1], tokens_of(k - 1)[:, c], preferred_element_type=F32)
            staged[k, :, :, :, c] = out.astype(BF16).reshape(OWN, PLANE, PAD, COLS)

        loop(nc, columns)

    def dispatch(k):
        loop(PLANE - 1, lambda i: slot_copy(k, PLANE - 1 - i).start())
        slots[k, :, place] = staged[k, :, place]

    def ffn(n, read, write):
        def up(i):
            g = n * nf + i
            s = g % DEEP_F
            for c in f_copies(s_gate, s_up, 0, s):
                c.wait()
            z = read()
            a = jnp.dot(z, fbuf[s, 0], preferred_element_type=F32)
            b = jnp.dot(z, fbuf[s, 1], preferred_element_type=F32)
            hidden[:, pl.ds(pl.multiple_of(i * WIDE, WIDE), WIDE)] = (a * jax.nn.sigmoid(a) * b).astype(BF16)
            start_f(g + DEEP_F)

        def down(i):
            g = n * nd + i
            s = g % DEEP_D
            d_copy(s_down, 0, s).wait()
            write(
                pl.ds(pl.multiple_of(i * WIDE, WIDE), WIDE),
                jnp.dot(hidden[...], dbuf[s], preferred_element_type=F32),
            )
            start_d(g + DEEP_D)

        scoped("up", lambda: loop(nf, up))
        scoped("down", lambda: loop(whole, down))
        if tail:
            g = n * nd + whole
            s = g % DEEP_D
            d_tail(s_down, s).wait()
            write(
                pl.ds(whole * WIDE, tail),
                jnp.dot(hidden[...], dbuf[s, :, 0:tail], preferred_element_type=F32),
            )
            start_d(g + DEEP_D)

    def back_copy(p, j):
        k, r, rows = BACK[p]
        device, there = peer(j)
        return pltpu.make_async_remote_copy(
            src_ref=staged.at[k, :, there, r : r + rows], dst_ref=back.at[k, :, place, r : r + rows],
            send_sem=r_send.at[p, j], recv_sem=r_recv.at[p, j], device_id=device, device_id_type=MESH,
        )

    def send_back(p):
        loop(PLANE - 1, lambda i: back_copy(p, PLANE - 1 - i).start())
        k, r, rows = BACK[p]
        back[k, :, place, r : r + rows] = staged[k, :, place, r : r + rows]

    def term_copy(o, to, slot):
        return pltpu.make_async_remote_copy(
            src_ref=lines.at[o - 1], dst_ref=terms.at[slot], send_sem=p_send.at[o - 1], recv_sem=p_recv.at[slot],
            device_id=line_peer(to), device_id_type=MESH,
        )

    def term_wait(slot):
        term_copy(1, 1, slot).wait_recv()

    for k in range(LINE - 1):
        back[k, :, :, ROWS[k] : PAD] = jnp.zeros((OWN, PLANE, PAD - ROWS[k], depth), BF16)

    stage(0)
    scoped("barrier", lambda: pl.semaphore_wait(barrier, LINE - 1 + PLANE - 1))
    line_start(0)

    @pl.when(middle)
    def _():
        line_start(1)

    dispatch(0)

    def write_shared(c, value):
        shared[:, c] = value

    ffn(0, lambda: x[...], write_shared)
    scoped("wait_line1", lambda: line_wait(1))

    @pl.when(middle)
    def _():
        line_start(2)
        scoped("wait_line3m", lambda: line_wait(3))
        line_start(3)

    stage(1)
    dispatch(1)

    def call(m):
        n = m + 1
        k, e = m // OWN, m % OWN
        for kk in range(LINE):
            @pl.when(m == kk * OWN)
            def _():
                def wait(i):
                    c = slot_copy(kk, i + 1)
                    c.wait_recv()
                    c.wait_send()

                scoped(f"wait_slots{kk}", lambda: loop(PLANE - 1, wait))

        def write(c, value):
            staged[k, e, :, :, c] = value.astype(BF16).reshape(PLANE, PAD, value.shape[1])

        ffn(n, lambda: slots[k, e].reshape(PLANE * PAD, depth), write)

        @pl.when(m == 1)
        def _():
            scoped("wait_line2", lambda: line_wait(2))

            @pl.when(middle)
            def _():
                line_start(4)

            stage(2)
            dispatch(2)

        @pl.when(m == 4)
        def _():
            @pl.when((mz == 0) | (mz == 3))
            def _():
                scoped("wait_line3e", lambda: line_wait(3))

            stage(3)
            dispatch(3)

        @pl.when(m == 8)
        def _():
            send_back(2)

    loop(LINE * OWN, call)
    for p in (3, 4, 1, 0):
        send_back(p)

    def combine(o, pieces, write, wait=lambda: None):
        build(pick.at[0], PAD, o, START[o], ROWS[o], True)
        if o < LINE - 1:
            build(pick_next, HALF, o, START[o + 1], HALF, True)
        for p in pieces:
            scoped(f"wait_back{p}", lambda: loop(PLANE - 1, lambda i: back_copy(p, i + 1).wait_recv()))
        scoped(f"wait_terms{o}", wait)

        def columns(i):
            c = pl.ds(pl.multiple_of(i * COLS, COLS), COLS)

            def dot(weights, rows):
                return lax.dot_general(weights, rows, (((0,), (0,)), ((), ())), preferred_element_type=F32)

            out = dot(pick[0], back[o, :, :, :, c].reshape(BLOCKS * PAD, COLS))
            if o < LINE - 1:
                out += dot(pick_next[...], back[o + 1, :, :, 0:HALF, c].reshape(BLOCKS * HALF, COLS))
            write(c, out)

        loop(nc, columns)

    def pass_on(o, pieces, to, slot, add=None):
        def write(c, value):
            if add is not None:
                value += terms[add, :, c].astype(F32)
            lines[o - 1, :, c] = value.astype(BF16)

        combine(o, pieces, write, lambda: None if add is None else term_wait(add))
        term_copy(o, to, slot).start()

    for c in line_copies(0, *LINE_SENDS[0]):
        c.wait_send()

    @pl.when(middle)
    def _():
        for q in range(1, len(LINE_SENDS)):
            for c in line_copies(q, *LINE_SENDS[q]):
                c.wait_send()

    @pl.when((mz == 0) | (mz == 3))
    def _():
        pass_on(2, (2, 3), 1, 3)
        pass_on(3, (4,), 1, 1)

    @pl.when(middle)
    def _():
        pass_on(3, (2, 3, 4), 3, 2, 3)
        pass_on(2, (), 2, 1, 1)

    pass_on(1, (1,), 1, 0)

    def stay(c, value):
        shared[:, c] += value

    combine(0, (0,), stay)
    far = 1 + ((mz + 1) // 2) % 2
    scoped("wait_term_near", lambda: term_wait(0))
    scoped("wait_term_far", lambda: term_wait(far))

    def finish(i):
        c = pl.ds(pl.multiple_of(i * COLS, COLS), COLS)
        y[:, c] = (shared[:, c] + terms[0, :, c].astype(F32) + terms[far, :, c].astype(F32)).astype(BF16)

    loop(nc, finish)
    for o in range(1, LINE):
        term_copy(o, 1, 0).wait_send()
    for p in range(len(BACK)):
        loop(PLANE - 1, lambda i: back_copy(p, i + 1).wait_send())


def solution(mesh):
    def step(x, expert, slot, gate, w_gate, w_up, w_down, s_gate, s_up, s_down):
        tokens, depth = x.shape[2:]
        width = s_gate.shape[1]
        dev, e = expert[0, 0] // OWN, expert[0, 0] % OWN
        place = (dev // 8) * 2 + dev % 2
        code = ((dev // 2) % 4) * 1024 + (e * PLANE + place) * SLOTS + slot[0, 0]
        code = jnp.where(slot[0, 0] < SLOTS, code, -1)
        tab = jnp.concatenate([code.T.astype(F32), gate[0, 0].T], axis=0)
        vmem = pl.BlockSpec(memory_space=pltpu.VMEM)
        hbm = pl.BlockSpec(memory_space=pl.ANY)
        dma = pltpu.SemaphoreType.DMA
        rows = PLANE * PAD
        y = pl.pallas_call(
            kernel,
            name="moe",
            out_shape=jax.ShapeDtypeStruct((tokens, depth), BF16),
            in_specs=[vmem, vmem] + [hbm] * 6,
            out_specs=vmem,
            scratch_shapes=[
                pltpu.VMEM((LINE - 1, tokens, depth), BF16),
                pltpu.VMEM((LINE - 1, 16, tokens), F32),
                pltpu.VMEM((LINE, OWN, PLANE, PAD, depth), BF16),
                pltpu.VMEM((LINE, OWN, PLANE, PAD, depth), BF16),
                pltpu.VMEM((LINE, OWN, PLANE, PAD, depth), BF16),
                pltpu.VMEM((LINE, tokens, depth), BF16),
                pltpu.VMEM((tokens, depth), F32),
                pltpu.VMEM((rows, width), BF16),
                pltpu.VMEM((2, BLOCKS * PAD, tokens), BF16),
                pltpu.VMEM((BLOCKS * HALF, tokens), BF16),
                pltpu.VMEM((DEEP_F, 2, depth, WIDE), BF16),
                pltpu.VMEM((DEEP_D, width, WIDE), BF16),
                dma((5, 2)), dma((LINE - 1, 2)),
                dma((LINE, PLANE)), dma((LINE, PLANE)),
                dma((len(BACK), PLANE)), dma((len(BACK), PLANE)),
                dma((LINE - 1,)), dma((LINE,)),
                dma((DEEP_F, 2)), dma((DEEP_D,)),
            ],
            compiler_params=pltpu.CompilerParams(
                collective_id=0, has_side_effects=True, vmem_limit_bytes=67043328
            ),
        )(x[0, 0], tab, w_gate, w_up, w_down, s_gate, s_up, s_down)
        return y[None, None]

    row = P("dp", "ep", None, None)
    w = P("ep", None, None)
    s = P(None, None)
    return jax.shard_map(
        step, mesh=mesh, in_specs=(row, row, row, row, w, w, w, s, s, s), out_specs=row, check_vma=False
    )
```

```python
import functools

import jax
import jax.numpy as jnp
from jax import lax
from jax.experimental import pallas as pl
from jax.experimental.pallas import tpu as pltpu
from jax.sharding import PartitionSpec as P

F32, BF16, I32 = jnp.float32, jnp.bfloat16, jnp.int32
MESH = pl.DeviceIdType.MESH

SLOTS = 26
PLANE = 8
LINE = 4
OWN = 3
BLOCKS = OWN * PLANE
PAD = 32
START = (0, 24, 48, 72)
ROWS = (24, 24, 24, 32)
BACK = ((0, 0, 24), (1, 0, 24), (2, 0, 24), (3, 0, 16), (3, 16, 16))
HALF = 16
COLS = 256
WIDE = 512
DEEP_F, DEEP_D = 3, 3
CALLS = 1 + LINE * OWN


def loop(n, body):
    lax.fori_loop(0, n, lambda i, c: (body(i), c)[1], 0)


def kernel(
    x, tab, w_gate, w_up, w_down, s_gate, s_up, s_down, y,
    lines, tabs, staged, slots, back, terms, shared, hidden, pick, pick_next, fbuf, dbuf,
    z_send, z_recv, d_send, d_recv, r_send, r_recv, p_send, p_recv, f_sem, d_sem,
):
    me = lax.axis_index("ep")
    mx, my, mz, mc = me // 16, (me // 8) % 2, (me // 2) % 4, me % 2
    place = (me // 8) * 2 + mc
    depth = x.shape[1]
    nf, nc = s_gate.shape[1] // WIDE, depth // COLS
    whole, tail = depth // WIDE, depth % WIDE
    nd = whole + (tail > 0)
    middle = (mz > 0) & (mz < 3)

    def peer(j):
        px, py, pc = (mx + j // 4) % 2, (my + (j // 2) % 2) % 2, (mc + j % 2) % 2
        return {"ep": ((px * 2 + py) * 4 + mz) * 2 + pc}, (px * 2 + py) * 2 + pc

    def line_peer(o):
        pz = (mz + 1 - 2 * (mz % 2), (mz + 2) % 4, 3 - mz)[o - 1]
        return {"ep": ((mx * 2 + my) * 4 + pz) * 2 + mc}

    def wide(ref, i):
        return ref.at[:, pl.ds(pl.multiple_of(i * WIDE, WIDE), WIDE)]

    def d_copy(ref, i, s):
        return pltpu.make_async_copy(wide(ref, i), dbuf.at[s], d_sem.at[s])

    def d_tail(ref, s):
        return pltpu.make_async_copy(ref.at[:, whole * WIDE :], dbuf.at[s, :, 0:tail], d_sem.at[s])

    def f_copies(gate, up, i, s):
        return [
            pltpu.make_async_copy(wide(gate, i), fbuf.at[s, 0], f_sem.at[s, 0]),
            pltpu.make_async_copy(wide(up, i), fbuf.at[s, 1], f_sem.at[s, 1]),
        ]

    def start_f(g):
        n, i, s = g // nf, g % nf, g % DEEP_F

        @pl.when(n == 0)
        def _():
            for c in f_copies(s_gate, s_up, i, s):
                c.start()

        @pl.when((n > 0) & (n < CALLS))
        def _():
            e = (n + OWN - 1) % OWN
            for c in f_copies(w_gate.at[e], w_up.at[e], i, s):
                c.start()

    def start_d(g):
        n, i, s = g // nd, g % nd, g % DEEP_D

        def start(ref):
            @pl.when(i < whole)
            def _():
                d_copy(ref, i, s).start()

            if tail:
                @pl.when(i == whole)
                def _():
                    d_tail(ref, s).start()

        @pl.when(n == 0)
        def _():
            start(s_down)

        @pl.when((n > 0) & (n < CALLS))
        def _():
            start(w_down.at[(n + OWN - 1) % OWN])

    loop(DEEP_F, start_f)
    loop(DEEP_D, start_d)

    barrier = pltpu.get_barrier_semaphore()
    for o in range(1, LINE):
        pl.semaphore_signal(barrier, inc=1, device_id=line_peer(o), device_id_type=MESH)
    for j in range(1, PLANE):
        pl.semaphore_signal(barrier, inc=1, device_id=peer(j)[0], device_id_type=MESH)
    def line_copies(q, src, to, slot):
        pairs = ((tab, x),) + tuple((tabs.at[o], lines.at[o]) for o in range(LINE - 1))
        return [
            pltpu.make_async_remote_copy(
                src_ref=ref, dst_ref=dst.at[slot - 1], send_sem=z_send.at[q, i], recv_sem=z_recv.at[slot - 1, i],
                device_id=line_peer(to), device_id_type=MESH,
            )
            for i, (ref, dst) in enumerate(zip(pairs[src], (tabs, lines)))
        ]

    LINE_SENDS = ((0, 1, 1), (0, 3, 3), (1, 3, 2), (3, 1, 2), (2, 1, 3))

    def line_start(q):
        for c in line_copies(q, *LINE_SENDS[q]):
            c.start()

    def line_wait(o):
        for c in line_copies(0, 0, o, o):
            c.wait_recv()

    def build(ref, height, o, start, rows, weigh):
        table = tab if o == 0 else tabs.at[o - 1]
        code = table[0:8, :].astype(I32) - mz * 1024
        gates = table[8:16, :]
        r = lax.broadcasted_iota(I32, (height, code.shape[1]), 0)
        v = r + (start - SLOTS * o)
        ok = (v >= 0) & (v < SLOTS) & (r < rows)

        def block(b):
            want = jnp.where(ok, v + b * SLOTS, -7)
            acc = jnp.zeros(want.shape, F32)
            for i in range(8):
                value = gates[i : i + 1, :] if weigh else jnp.float32(1)
                acc = jnp.where(want == code[i : i + 1, :], value, acc)
            ref[pl.ds(pl.multiple_of(b * height, height), height), :] = acc.astype(BF16)

        loop(BLOCKS, block)

    def tokens_of(o):
        return x if o == 0 else lines.at[o - 1]

    def slot_copy(k, j):
        device, there = peer(j)
        return pltpu.make_async_remote_copy(
            src_ref=staged.at[k, :, there, 0 : ROWS[k]], dst_ref=slots.at[k, :, place, 0 : ROWS[k]],
            send_sem=d_send.at[k, j], recv_sem=d_recv.at[k, j], device_id=device, device_id_type=MESH,
        )

    def stage(k):
        build(pick.at[0], PAD, k, START[k], ROWS[k], False)
        if k:
            build(pick.at[1], PAD, k - 1, START[k], ROWS[k], False)

        def columns(i):
            c = pl.ds(pl.multiple_of(i * COLS, COLS), COLS)
            out = jnp.dot(pick[0], tokens_of(k)[:, c], preferred_element_type=F32)
            if k:
                out += jnp.dot(pick[1], tokens_of(k - 1)[:, c], preferred_element_type=F32)
            staged[k, :, :, :, c] = out.astype(BF16).reshape(OWN, PLANE, PAD, COLS)

        loop(nc, columns)

    def dispatch(k):
        loop(PLANE - 1, lambda i: slot_copy(k, PLANE - 1 - i).start())
        slots[k, :, place] = staged[k, :, place]

    def ffn(n, read, write):
        def up(i):
            g = n * nf + i
            s = g % DEEP_F
            for c in f_copies(s_gate, s_up, 0, s):
                c.wait()
            z = read()
            a = jnp.dot(z, fbuf[s, 0], preferred_element_type=F32)
            b = jnp.dot(z, fbuf[s, 1], preferred_element_type=F32)
            hidden[:, pl.ds(pl.multiple_of(i * WIDE, WIDE), WIDE)] = (a * jax.nn.sigmoid(a) * b).astype(BF16)
            start_f(g + DEEP_F)

        def down(i):
            g = n * nd + i
            s = g % DEEP_D
            d_copy(s_down, 0, s).wait()
            write(
                pl.ds(pl.multiple_of(i * WIDE, WIDE), WIDE),
                jnp.dot(hidden[...], dbuf[s], preferred_element_type=F32),
            )
            start_d(g + DEEP_D)

        loop(nf, up)
        loop(whole, down)
        if tail:
            g = n * nd + whole
            s = g % DEEP_D
            d_tail(s_down, s).wait()
            write(
                pl.ds(whole * WIDE, tail),
                jnp.dot(hidden[...], dbuf[s, :, 0:tail], preferred_element_type=F32),
            )
            start_d(g + DEEP_D)

    def back_copy(p, j):
        k, r, rows = BACK[p]
        device, there = peer(j)
        return pltpu.make_async_remote_copy(
            src_ref=staged.at[k, :, there, r : r + rows], dst_ref=back.at[k, :, place, r : r + rows],
            send_sem=r_send.at[p, j], recv_sem=r_recv.at[p, j], device_id=device, device_id_type=MESH,
        )

    def send_back(p):
        loop(PLANE - 1, lambda i: back_copy(p, PLANE - 1 - i).start())
        k, r, rows = BACK[p]
        back[k, :, place, r : r + rows] = staged[k, :, place, r : r + rows]

    def term_copy(o, to, slot):
        return pltpu.make_async_remote_copy(
            src_ref=lines.at[o - 1], dst_ref=terms.at[slot], send_sem=p_send.at[o - 1], recv_sem=p_recv.at[slot],
            device_id=line_peer(to), device_id_type=MESH,
        )

    def term_wait(slot):
        term_copy(1, 1, slot).wait_recv()

    for k in range(LINE - 1):
        back[k, :, :, ROWS[k] : PAD] = jnp.zeros((OWN, PLANE, PAD - ROWS[k], depth), BF16)

    stage(0)
    pl.semaphore_wait(barrier, LINE - 1 + PLANE - 1)
    line_start(0)

    @pl.when(middle)
    def _():
        line_start(1)

    dispatch(0)

    def write_shared(c, value):
        shared[:, c] = value

    ffn(0, lambda: x[...], write_shared)
    line_wait(1)

    @pl.when(middle)
    def _():
        line_start(2)
        line_wait(3)
        line_start(3)

    stage(1)
    dispatch(1)

    def call(m):
        n = m + 1
        k, e = m // OWN, m % OWN
        for kk in range(LINE):
            @pl.when(m == kk * OWN)
            def _():
                def wait(i):
                    c = slot_copy(kk, i + 1)
                    c.wait_recv()
                    c.wait_send()

                loop(PLANE - 1, wait)

        def write(c, value):
            staged[k, e, :, :, c] = value.astype(BF16).reshape(PLANE, PAD, value.shape[1])

        ffn(n, lambda: slots[k, e].reshape(PLANE * PAD, depth), write)

        @pl.when(m == 1)
        def _():
            line_wait(2)

            @pl.when(middle)
            def _():
                line_start(4)

            stage(2)
            dispatch(2)

        @pl.when(m == 4)
        def _():
            @pl.when((mz == 0) | (mz == 3))
            def _():
                line_wait(3)

            stage(3)
            dispatch(3)

        @pl.when(m == 8)
        def _():
            send_back(2)

    loop(LINE * OWN, call)
    for p in (3, 4, 1, 0):
        send_back(p)

    def combine(o, pieces, write, wait=lambda: None):
        build(pick.at[0], PAD, o, START[o], ROWS[o], True)
        if o < LINE - 1:
            build(pick_next, HALF, o, START[o + 1], HALF, True)
        for p in pieces:
            loop(PLANE - 1, lambda i: back_copy(p, i + 1).wait_recv())
        wait()

        def columns(i):
            c = pl.ds(pl.multiple_of(i * COLS, COLS), COLS)

            def dot(weights, rows):
                return lax.dot_general(weights, rows, (((0,), (0,)), ((), ())), preferred_element_type=F32)

            out = dot(pick[0], back[o, :, :, :, c].reshape(BLOCKS * PAD, COLS))
            if o < LINE - 1:
                out += dot(pick_next[...], back[o + 1, :, :, 0:HALF, c].reshape(BLOCKS * HALF, COLS))
            write(c, out)

        loop(nc, columns)

    def pass_on(o, pieces, to, slot, add=None):
        def write(c, value):
            if add is not None:
                value += terms[add, :, c].astype(F32)
            lines[o - 1, :, c] = value.astype(BF16)

        combine(o, pieces, write, lambda: None if add is None else term_wait(add))
        term_copy(o, to, slot).start()

    for c in line_copies(0, *LINE_SENDS[0]):
        c.wait_send()

    @pl.when(middle)
    def _():
        for q in range(1, len(LINE_SENDS)):
            for c in line_copies(q, *LINE_SENDS[q]):
                c.wait_send()

    @pl.when((mz == 0) | (mz == 3))
    def _():
        pass_on(2, (2, 3), 1, 3)
        pass_on(3, (4,), 3, 2)

    @pl.when(middle)
    def _():
        pass_on(2, (2, 3), 2, 1)
        pass_on(3, (4,), 3, 2, 3)

    pass_on(1, (1,), 1, 0)

    @pl.when((mz == 0) | (mz == 3))
    def _():
        term_wait(1)

        def add(i):
            c = pl.ds(pl.multiple_of(i * COLS, COLS), COLS)
            shared[:, c] += terms[1, :, c].astype(F32)

        loop(nc, add)

    def stay(c, value):
        shared[:, c] += value

    combine(0, (0,), stay)
    term_wait(2)
    term_wait(0)

    def finish(i):
        c = pl.ds(pl.multiple_of(i * COLS, COLS), COLS)
        y[:, c] = (shared[:, c] + terms[0, :, c].astype(F32) + terms[2, :, c].astype(F32)).astype(BF16)

    loop(nc, finish)
    for o in range(1, LINE):
        term_copy(o, 1, 0).wait_send()
    for p in range(len(BACK)):
        loop(PLANE - 1, lambda i: back_copy(p, i + 1).wait_send())


def solution(mesh):
    def step(x, expert, slot, gate, w_gate, w_up, w_down, s_gate, s_up, s_down):
        tokens, depth = x.shape[2:]
        width = s_gate.shape[1]
        dev, e = expert[0, 0] // OWN, expert[0, 0] % OWN
        place = (dev // 8) * 2 + dev % 2
        code = ((dev // 2) % 4) * 1024 + (e * PLANE + place) * SLOTS + slot[0, 0]
        code = jnp.where(slot[0, 0] < SLOTS, code, -1)
        tab = jnp.concatenate([code.T.astype(F32), gate[0, 0].T], axis=0)
        vmem = pl.BlockSpec(memory_space=pltpu.VMEM)
        hbm = pl.BlockSpec(memory_space=pl.ANY)
        dma = pltpu.SemaphoreType.DMA
        rows = PLANE * PAD
        y = pl.pallas_call(
            kernel,
            name="moe",
            out_shape=jax.ShapeDtypeStruct((tokens, depth), BF16),
            in_specs=[vmem, vmem] + [hbm] * 6,
            out_specs=vmem,
            scratch_shapes=[
                pltpu.VMEM((LINE - 1, tokens, depth), BF16),
                pltpu.VMEM((LINE - 1, 16, tokens), F32),
                pltpu.VMEM((LINE, OWN, PLANE, PAD, depth), BF16),
                pltpu.VMEM((LINE, OWN, PLANE, PAD, depth), BF16),
                pltpu.VMEM((LINE, OWN, PLANE, PAD, depth), BF16),
                pltpu.VMEM((LINE, tokens, depth), BF16),
                pltpu.VMEM((tokens, depth), F32),
                pltpu.VMEM((rows, width), BF16),
                pltpu.VMEM((2, BLOCKS * PAD, tokens), BF16),
                pltpu.VMEM((BLOCKS * HALF, tokens), BF16),
                pltpu.VMEM((DEEP_F, 2, depth, WIDE), BF16),
                pltpu.VMEM((DEEP_D, width, WIDE), BF16),
                dma((5, 2)), dma((LINE - 1, 2)),
                dma((LINE, PLANE)), dma((LINE, PLANE)),
                dma((len(BACK), PLANE)), dma((len(BACK), PLANE)),
                dma((LINE - 1,)), dma((LINE,)),
                dma((DEEP_F, 2)), dma((DEEP_D,)),
            ],
            compiler_params=pltpu.CompilerParams(
                collective_id=0, has_side_effects=True, vmem_limit_bytes=67043328
            ),
        )(x[0, 0], tab, w_gate, w_up, w_down, s_gate, s_up, s_down)
        return y[None, None]

    row = P("dp", "ep", None, None)
    w = P("ep", None, None)
    s = P(None, None)
    return jax.shard_map(
        step, mesh=mesh, in_specs=(row, row, row, row, w, w, w, s, s, s), out_specs=row, check_vma=False
    )
```

```python
import functools

import jax
import jax.numpy as jnp
from jax import lax
from jax.experimental import pallas as pl
from jax.experimental.pallas import tpu as pltpu
from jax.sharding import PartitionSpec as P

F32, BF16, I32 = jnp.float32, jnp.bfloat16, jnp.int32
MESH = pl.DeviceIdType.MESH

SLOTS = 26
PLANE = 8
LINE = 4
OWN = 3
BLOCKS = OWN * PLANE
PAD = 32
START = (0, 24, 48, 72)
ROWS = (24, 24, 24, 32)
BACK = ((0, 0, 24), (1, 0, 24), (2, 0, 24), (3, 0, 16), (3, 16, 16))
HALF = 16
COLS = 256
WIDE = 512
DEEP_F, DEEP_D = 3, 3
CALLS = 1 + LINE * OWN


def loop(n, body):
    lax.fori_loop(0, n, lambda i, c: (body(i), c)[1], 0)


def kernel(
    x, tab, w_gate, w_up, w_down, s_gate, s_up, s_down, y,
    lines, tabs, staged, slots, back, terms, shared, hidden, pick, pick_next, fbuf, dbuf,
    z_send, z_recv, d_send, d_recv, r_send, r_recv, p_send, p_recv, f_sem, d_sem,
):
    me = lax.axis_index("ep")
    mx, my, mz, mc = me // 16, (me // 8) % 2, (me // 2) % 4, me % 2
    place = (me // 8) * 2 + mc
    depth = x.shape[1]
    nf, nc = s_gate.shape[1] // WIDE, depth // COLS
    whole, tail = depth // WIDE, depth % WIDE
    nd = whole + (tail > 0)
    middle = (mz > 0) & (mz < 3)

    def peer(j):
        px, py, pc = (mx + j // 4) % 2, (my + (j // 2) % 2) % 2, (mc + j % 2) % 2
        return {"ep": ((px * 2 + py) * 4 + mz) * 2 + pc}, (px * 2 + py) * 2 + pc

    def line_peer(o):
        pz = (mz + 1 - 2 * (mz % 2), (mz + 2) % 4, 3 - mz)[o - 1]
        return {"ep": ((mx * 2 + my) * 4 + pz) * 2 + mc}

    def wide(ref, i):
        return ref.at[:, pl.ds(pl.multiple_of(i * WIDE, WIDE), WIDE)]

    def d_copy(ref, i, s):
        return pltpu.make_async_copy(wide(ref, i), dbuf.at[s], d_sem.at[s])

    def d_tail(ref, s):
        return pltpu.make_async_copy(ref.at[:, whole * WIDE :], dbuf.at[s, :, 0:tail], d_sem.at[s])

    def f_copies(gate, up, i, s):
        return [
            pltpu.make_async_copy(wide(gate, i), fbuf.at[s, 0], f_sem.at[s, 0]),
            pltpu.make_async_copy(wide(up, i), fbuf.at[s, 1], f_sem.at[s, 1]),
        ]

    def start_f(g):
        n, i, s = g // nf, g % nf, g % DEEP_F

        @pl.when(n == 0)
        def _():
            for c in f_copies(s_gate, s_up, i, s):
                c.start()

        @pl.when((n > 0) & (n < CALLS))
        def _():
            e = (n + OWN - 1) % OWN
            for c in f_copies(w_gate.at[e], w_up.at[e], i, s):
                c.start()

    def start_d(g):
        n, i, s = g // nd, g % nd, g % DEEP_D

        def start(ref):
            @pl.when(i < whole)
            def _():
                d_copy(ref, i, s).start()

            if tail:
                @pl.when(i == whole)
                def _():
                    d_tail(ref, s).start()

        @pl.when(n == 0)
        def _():
            start(s_down)

        @pl.when((n > 0) & (n < CALLS))
        def _():
            start(w_down.at[(n + OWN - 1) % OWN])

    loop(DEEP_F, start_f)
    loop(DEEP_D, start_d)

    barrier = pltpu.get_barrier_semaphore()
    for o in range(1, LINE):
        pl.semaphore_signal(barrier, inc=1, device_id=line_peer(o), device_id_type=MESH)
    for j in range(1, PLANE):
        pl.semaphore_signal(barrier, inc=1, device_id=peer(j)[0], device_id_type=MESH)
    def line_copies(q, src, to, slot):
        pairs = ((tab, x),) + tuple((tabs.at[o], lines.at[o]) for o in range(LINE - 1))
        return [
            pltpu.make_async_remote_copy(
                src_ref=ref, dst_ref=dst.at[slot - 1], send_sem=z_send.at[q, i], recv_sem=z_recv.at[slot - 1, i],
                device_id=line_peer(to), device_id_type=MESH,
            )
            for i, (ref, dst) in enumerate(zip(pairs[src], (tabs, lines)))
        ]

    LINE_SENDS = ((0, 1, 1), (0, 3, 3), (1, 3, 2), (3, 1, 2), (2, 1, 3))

    def line_start(q):
        for c in line_copies(q, *LINE_SENDS[q]):
            c.start()

    def line_wait(o):
        for c in line_copies(0, 0, o, o):
            c.wait_recv()

    def build(ref, height, o, start, rows, weigh):
        table = tab if o == 0 else tabs.at[o - 1]
        code = table[0:8, :].astype(I32) - mz * 1024
        gates = table[8:16, :]
        r = lax.broadcasted_iota(I32, (height, code.shape[1]), 0)
        v = r + (start - SLOTS * o)
        ok = (v >= 0) & (v < SLOTS) & (r < rows)

        def block(b):
            want = jnp.where(ok, v + b * SLOTS, -7)
            acc = jnp.zeros(want.shape, F32)
            for i in range(8):
                value = gates[i : i + 1, :] if weigh else jnp.float32(1)
                acc = jnp.where(want == code[i : i + 1, :], value, acc)
            ref[pl.ds(pl.multiple_of(b * height, height), height), :] = acc.astype(BF16)

        loop(BLOCKS, block)

    def tokens_of(o):
        return x if o == 0 else lines.at[o - 1]

    def slot_copy(k, j):
        device, there = peer(j)
        return pltpu.make_async_remote_copy(
            src_ref=staged.at[k, :, there, 0 : ROWS[k]], dst_ref=slots.at[k, :, place, 0 : ROWS[k]],
            send_sem=d_send.at[k, j], recv_sem=d_recv.at[k, j], device_id=device, device_id_type=MESH,
        )

    def early(k):
        build(pick.at[1], PAD, k - 1, START[k], ROWS[k], False)

        def columns(i):
            c = pl.ds(pl.multiple_of(i * COLS, COLS), COLS)
            out = jnp.dot(pick[1], tokens_of(k - 1)[:, c], preferred_element_type=F32)
            staged[k, :, :, :, c] = out.astype(BF16).reshape(OWN, PLANE, PAD, COLS)

        loop(nc, columns)

    def stage(k):
        build(pick.at[0], PAD, k, START[k], ROWS[k], False)
        if k == LINE - 1:
            build(pick.at[1], PAD, k - 1, START[k], ROWS[k], False)

        def columns(i):
            c = pl.ds(pl.multiple_of(i * COLS, COLS), COLS)
            out = jnp.dot(pick[0], tokens_of(k)[:, c], preferred_element_type=F32)
            if k == LINE - 1:
                out += jnp.dot(pick[1], tokens_of(k - 1)[:, c], preferred_element_type=F32)
            elif k:
                out += staged[k, :, :, :, c].reshape(BLOCKS * PAD, COLS).astype(F32)
            staged[k, :, :, :, c] = out.astype(BF16).reshape(OWN, PLANE, PAD, COLS)

        loop(nc, columns)

    def dispatch(k):
        loop(PLANE - 1, lambda i: slot_copy(k, PLANE - 1 - i).start())
        slots[k, :, place] = staged[k, :, place]

    def ffn(n, read, write):
        def up(i):
            g = n * nf + i
            s = g % DEEP_F
            for c in f_copies(s_gate, s_up, 0, s):
                c.wait()
            z = read()
            a = jnp.dot(z, fbuf[s, 0], preferred_element_type=F32)
            b = jnp.dot(z, fbuf[s, 1], preferred_element_type=F32)
            hidden[:, pl.ds(pl.multiple_of(i * WIDE, WIDE), WIDE)] = (a * jax.nn.sigmoid(a) * b).astype(BF16)
            start_f(g + DEEP_F)

        def down(i):
            g = n * nd + i
            s = g % DEEP_D
            d_copy(s_down, 0, s).wait()
            write(
                pl.ds(pl.multiple_of(i * WIDE, WIDE), WIDE),
                jnp.dot(hidden[...], dbuf[s], preferred_element_type=F32),
            )
            start_d(g + DEEP_D)

        loop(nf, up)
        loop(whole, down)
        if tail:
            g = n * nd + whole
            s = g % DEEP_D
            d_tail(s_down, s).wait()
            write(
                pl.ds(whole * WIDE, tail),
                jnp.dot(hidden[...], dbuf[s, :, 0:tail], preferred_element_type=F32),
            )
            start_d(g + DEEP_D)

    def back_copy(p, j):
        k, r, rows = BACK[p]
        device, there = peer(j)
        return pltpu.make_async_remote_copy(
            src_ref=staged.at[k, :, there, r : r + rows], dst_ref=back.at[k, :, place, r : r + rows],
            send_sem=r_send.at[p, j], recv_sem=r_recv.at[p, j], device_id=device, device_id_type=MESH,
        )

    def send_back(p):
        loop(PLANE - 1, lambda i: back_copy(p, PLANE - 1 - i).start())
        k, r, rows = BACK[p]
        back[k, :, place, r : r + rows] = staged[k, :, place, r : r + rows]

    def term_copy(o, to, slot):
        return pltpu.make_async_remote_copy(
            src_ref=lines.at[o - 1], dst_ref=terms.at[slot], send_sem=p_send.at[o - 1], recv_sem=p_recv.at[slot],
            device_id=line_peer(to), device_id_type=MESH,
        )

    def term_wait(slot):
        term_copy(1, 1, slot).wait_recv()

    for k in range(LINE - 1):
        back[k, :, :, ROWS[k] : PAD] = jnp.zeros((OWN, PLANE, PAD - ROWS[k], depth), BF16)

    stage(0)
    pl.semaphore_wait(barrier, LINE - 1 + PLANE - 1)
    line_start(0)

    @pl.when(middle)
    def _():
        line_start(1)

    dispatch(0)

    def write_shared(c, value):
        shared[:, c] = value

    ffn(0, lambda: x[...], write_shared)
    early(1)
    line_wait(1)

    @pl.when(middle)
    def _():
        line_start(2)
        line_wait(3)
        line_start(3)

    stage(1)
    dispatch(1)

    def call(m):
        n = m + 1
        k, e = m // OWN, m % OWN
        for kk in range(LINE):
            @pl.when(m == kk * OWN)
            def _():
                def wait(i):
                    c = slot_copy(kk, i + 1)
                    c.wait_recv()
                    c.wait_send()

                loop(PLANE - 1, wait)

        def write(c, value):
            staged[k, e, :, :, c] = value.astype(BF16).reshape(PLANE, PAD, value.shape[1])

        ffn(n, lambda: slots[k, e].reshape(PLANE * PAD, depth), write)

        @pl.when(m == 1)
        def _():
            early(2)
            line_wait(2)

            @pl.when(middle)
            def _():
                line_start(4)

            stage(2)
            dispatch(2)

        @pl.when(m == 4)
        def _():
            @pl.when((mz == 0) | (mz == 3))
            def _():
                line_wait(3)

            stage(3)
            dispatch(3)

        @pl.when(m == 8)
        def _():
            send_back(2)

    loop(LINE * OWN, call)
    for p in (3, 4, 1, 0):
        send_back(p)

    def combine(o, pieces, write, wait=lambda: None):
        build(pick.at[0], PAD, o, START[o], ROWS[o], True)
        if o < LINE - 1:
            build(pick_next, HALF, o, START[o + 1], HALF, True)
        for p in pieces:
            loop(PLANE - 1, lambda i: back_copy(p, i + 1).wait_recv())
        wait()

        def columns(i):
            c = pl.ds(pl.multiple_of(i * COLS, COLS), COLS)

            def dot(weights, rows):
                return lax.dot_general(weights, rows, (((0,), (0,)), ((), ())), preferred_element_type=F32)

            out = dot(pick[0], back[o, :, :, :, c].reshape(BLOCKS * PAD, COLS))
            if o < LINE - 1:
                out += dot(pick_next[...], back[o + 1, :, :, 0:HALF, c].reshape(BLOCKS * HALF, COLS))
            write(c, out)

        loop(nc, columns)

    def pass_on(o, pieces, to, slot, add=None):
        def write(c, value):
            if add is not None:
                value += terms[add, :, c].astype(F32)
            lines[o - 1, :, c] = value.astype(BF16)

        combine(o, pieces, write, lambda: None if add is None else term_wait(add))
        term_copy(o, to, slot).start()

    for c in line_copies(0, *LINE_SENDS[0]):
        c.wait_send()

    @pl.when(middle)
    def _():
        for q in range(1, len(LINE_SENDS)):
            for c in line_copies(q, *LINE_SENDS[q]):
                c.wait_send()

    @pl.when((mz == 0) | (mz == 3))
    def _():
        pass_on(2, (2, 3), 1, 3)
        pass_on(3, (4,), 3, 2)

    @pl.when(middle)
    def _():
        pass_on(2, (2, 3), 2, 1)
        pass_on(3, (4,), 3, 2, 3)

    pass_on(1, (1,), 1, 0)

    @pl.when((mz == 0) | (mz == 3))
    def _():
        term_wait(1)

        def add(i):
            c = pl.ds(pl.multiple_of(i * COLS, COLS), COLS)
            shared[:, c] += terms[1, :, c].astype(F32)

        loop(nc, add)

    def stay(c, value):
        shared[:, c] += value

    combine(0, (0,), stay)
    term_wait(2)
    term_wait(0)

    def finish(i):
        c = pl.ds(pl.multiple_of(i * COLS, COLS), COLS)
        y[:, c] = (shared[:, c] + terms[0, :, c].astype(F32) + terms[2, :, c].astype(F32)).astype(BF16)

    loop(nc, finish)
    for o in range(1, LINE):
        term_copy(o, 1, 0).wait_send()
    for p in range(len(BACK)):
        loop(PLANE - 1, lambda i: back_copy(p, i + 1).wait_send())


def solution(mesh):
    def step(x, expert, slot, gate, w_gate, w_up, w_down, s_gate, s_up, s_down):
        tokens, depth = x.shape[2:]
        width = s_gate.shape[1]
        dev, e = expert[0, 0] // OWN, expert[0, 0] % OWN
        place = (dev // 8) * 2 + dev % 2
        code = ((dev // 2) % 4) * 1024 + (e * PLANE + place) * SLOTS + slot[0, 0]
        code = jnp.where(slot[0, 0] < SLOTS, code, -1)
        tab = jnp.concatenate([code.T.astype(F32), gate[0, 0].T], axis=0)
        vmem = pl.BlockSpec(memory_space=pltpu.VMEM)
        hbm = pl.BlockSpec(memory_space=pl.ANY)
        dma = pltpu.SemaphoreType.DMA
        rows = PLANE * PAD
        y = pl.pallas_call(
            kernel,
            name="moe",
            out_shape=jax.ShapeDtypeStruct((tokens, depth), BF16),
            in_specs=[vmem, vmem] + [hbm] * 6,
            out_specs=vmem,
            scratch_shapes=[
                pltpu.VMEM((LINE - 1, tokens, depth), BF16),
                pltpu.VMEM((LINE - 1, 16, tokens), F32),
                pltpu.VMEM((LINE, OWN, PLANE, PAD, depth), BF16),
                pltpu.VMEM((LINE, OWN, PLANE, PAD, depth), BF16),
                pltpu.VMEM((LINE, OWN, PLANE, PAD, depth), BF16),
                pltpu.VMEM((LINE, tokens, depth), BF16),
                pltpu.VMEM((tokens, depth), F32),
                pltpu.VMEM((rows, width), BF16),
                pltpu.VMEM((2, BLOCKS * PAD, tokens), BF16),
                pltpu.VMEM((BLOCKS * HALF, tokens), BF16),
                pltpu.VMEM((DEEP_F, 2, depth, WIDE), BF16),
                pltpu.VMEM((DEEP_D, width, WIDE), BF16),
                dma((5, 2)), dma((LINE - 1, 2)),
                dma((LINE, PLANE)), dma((LINE, PLANE)),
                dma((len(BACK), PLANE)), dma((len(BACK), PLANE)),
                dma((LINE - 1,)), dma((LINE,)),
                dma((DEEP_F, 2)), dma((DEEP_D,)),
            ],
            compiler_params=pltpu.CompilerParams(
                collective_id=0, has_side_effects=True, vmem_limit_bytes=67043328
            ),
        )(x[0, 0], tab, w_gate, w_up, w_down, s_gate, s_up, s_down)
        return y[None, None]

    row = P("dp", "ep", None, None)
    w = P("ep", None, None)
    s = P(None, None)
    return jax.shard_map(
        step, mesh=mesh, in_specs=(row, row, row, row, w, w, w, s, s, s), out_specs=row, check_vma=False
    )
```
